32 devices in a mesh: parts: 2 (over y), gz: 4 (over z), shot: 4 (over x, core).
Axes of the slice: x: 2, y: 2, z: 4, core: 2. Of those that a mesh axis runs over, the one named last changes fastest.
Arguments:
- wavefields: float32 [8, 2, 9, 16, 32, 128], P(('parts', 'shot'), None, None, 'gz'), parts along dimension 0, may hold values from -6 to 6
- earth_model: float32 [6, 16, 32, 128], P('parts', 'gz'), parts along dimension 0, may hold values from 0.4 to 1.6
- source_depth: int32 [8], P(('parts', 'shot')), parts along dimension 0, may hold values from 0 to 15
- source_column: int32 [8], P(('parts', 'shot')), parts along dimension 0, may hold values from 0 to 4095
- wavelet: float32 [8, 8], P(('parts', 'shot')), parts along dimension 0, may hold values from -30 to 30
- receiver_depth: int32 [8, 64], P(('parts', 'shot')), parts along dimension 0, may hold values from 0 to 15
- receiver_column: int32 [8, 64], P(('parts', 'shot')), parts along dimension 0, may hold values from 0 to 4095
- traces: float32 [8, 8, 64], P(('parts', 'shot')), parts along dimension 0, may hold values from -30 to 30
Outputs:
- images: float32 [4, 16, 32, 128], P('parts', 'gz'), parts along dimension 0
The draws below stay inside these ranges and needn't reach their ends.
There are 2 independent parts, one for each index of `parts`. The reference program is written for one: setup_inputs(seed, part) draws one part's arguments, and reference() takes and returns one part's arrays. A program takes and returns all parts, laid end to end along the dimension named above; each array names one. Nothing has to cross between parts.
All inputs are finite; a program needn't handle non-finite values.
Results may differ from the reference program's by a relative error of at most 0.00002.
Values sent between devices are 32-bit elements; how exact they have to be, the bound alone decides.
A program may use at most 64 MiB of HBM per device.

```python
import math
import jax
import jax.numpy as jnp
from jax import lax

NX = 32
NY = 128
STEPS = 8
RECV = 64
NZ = 16
SHOTS = 4


def plant(drawn, key, smallest, top_value):
    dims = drawn.shape
    spot = [jax.random.randint(jax.random.fold_in(key, axis), (), 0, dims[axis]) for axis in range(len(dims))]
    drawn = drawn.at[tuple(spot)].set(smallest)
    longest = dims.index(max(dims))
    spot[longest] = (spot[longest] + 1) % dims[longest]
    return drawn.at[tuple(spot)].set(top_value)


def levels(stream_key, extent, pieces, least, top_value):
    loudness = 1.0
    for position, parts in pieces:
        heights = jax.random.uniform(jax.random.fold_in(jax.random.fold_in(stream_key, 6), position), (parts,), jnp.float32, least / len(pieces), top_value / len(pieces))
        loudness = loudness * jnp.repeat(jnp.exp(heights), extent[position] // parts).reshape((-1,) + (1,) * (len(extent) - 1 - position))
    return loudness


def noise(stream_key, shape, scale, most, cuts=(), held_as=jnp.bfloat16):
    result = scale * jax.random.normal(stream_key, shape, jnp.float32)
    if cuts:
        result = result * levels(stream_key, shape, cuts, -0.22, 0.18)
    return jnp.clip(result, -most, most).astype(held_as)


def setup_inputs(seed: int = 0, part: int = 0) -> dict:
    key_list = jax.random.split(jax.random.key(seed), 9)
    part_keys = jax.random.split(jax.random.fold_in(key_list[8], part), 9)
    return {
        "wavefields": noise(part_keys[0], (SHOTS, 2, 9, NZ, NX, NY), 1.0, 6.0, ((0, 4), (3, 4)), jnp.float32),
        "earth_model": jnp.clip(jnp.exp(math.log(1.6) - 1.3862944 * jax.random.uniform(part_keys[1], (3, NZ, NX, NY), jnp.float32) ** levels(part_keys[1], (3, NZ, NX, NY), ((1, 4),), -0.2, 0.2)), 0.4, 1.6),
        "source_depth": plant(jax.random.randint(part_keys[2], (SHOTS,), 0, NZ), jax.random.fold_in(part_keys[2], 1), 0, NZ - 1).astype(jnp.int32),
        "source_column": plant(jax.random.randint(part_keys[3], (SHOTS,), 0, NX * NY), jax.random.fold_in(part_keys[3], 1), 0, (NX * NY) - 1).astype(jnp.int32),
        "wavelet": noise(part_keys[4], (SHOTS, STEPS), 5.0, 30.0, ((0, 4),), jnp.float32),
        "receiver_depth": plant(jax.random.randint(part_keys[5], (SHOTS, RECV), 0, NZ), jax.random.fold_in(part_keys[5], 1), 0, NZ - 1).astype(jnp.int32),
        "receiver_column": plant(jax.random.randint(part_keys[6], (SHOTS, RECV), 0, NX * NY), jax.random.fold_in(part_keys[6], 1), 0, (NX * NY) - 1).astype(jnp.int32),
        "traces": noise(part_keys[7], (SHOTS, STEPS, RECV), 5.0, 30.0, ((0, 4),), jnp.float32),
    }


time_step = 0.15


def forward_diff(array, dim_index):
    length = array.shape[dim_index]
    following = jnp.concatenate([lax.slice_in_dim(array, 1, length, axis=dim_index), jnp.zeros_like(lax.slice_in_dim(array, 0, 1, axis=dim_index))], axis=dim_index)
    return following - array


def backward_diff(array, dim_index):
    length = array.shape[dim_index]
    previous = jnp.concatenate([jnp.zeros_like(lax.slice_in_dim(array, 0, 1, axis=dim_index)), lax.slice_in_dim(array, 0, length - 1, axis=dim_index)], axis=dim_index)
    return array - previous


def depth_forward(array, plane_high):
    following = jnp.concatenate([array[:, 1:], plane_high[:, None]], axis=1)
    return following - array


def depth_backward(array, plane_low):
    previous = jnp.concatenate([plane_low[:, None], array[:, :-1]], axis=1)
    return array - previous


def velocity_half(fields, buoyancy, sxz_low, syz_low, szz_high):
    vel_x, vel_y, vel_z, sig_xx, sig_yy, sig_zz, sig_xy, sig_xz, sig_yz = fields
    vel_x = vel_x + time_step * buoyancy * (forward_diff(sig_xx, 2) + backward_diff(sig_xy, 3) + depth_backward(sig_xz, sxz_low))
    vel_y = vel_y + time_step * buoyancy * (backward_diff(sig_xy, 2) + forward_diff(sig_yy, 3) + depth_backward(sig_yz, syz_low))
    vel_z = vel_z + time_step * buoyancy * (backward_diff(sig_xz, 2) + backward_diff(sig_yz, 3) + depth_forward(sig_zz, szz_high))
    return vel_x, vel_y, vel_z


def stress_half(fields, lame_lambda, shear_mu, vz_low, vx_high, vy_high):
    vel_x, vel_y, vel_z, sig_xx, sig_yy, sig_zz, sig_xy, sig_xz, sig_yz = fields
    strain_x = backward_diff(vel_x, 2)
    strain_y = backward_diff(vel_y, 3)
    strain_z = depth_backward(vel_z, vz_low)
    spread = strain_x + strain_y + strain_z
    sig_xx = sig_xx + time_step * (lame_lambda * spread + 2.0 * shear_mu * strain_x)
    sig_yy = sig_yy + time_step * (lame_lambda * spread + 2.0 * shear_mu * strain_y)
    sig_zz = sig_zz + time_step * (lame_lambda * spread + 2.0 * shear_mu * strain_z)
    vx_up = depth_forward(vel_x, vx_high)
    vy_up = depth_forward(vel_y, vy_high)
    vz_along_x = forward_diff(vel_z, 2)
    vz_along_y = forward_diff(vel_z, 3)
    vx_along_y = forward_diff(vel_x, 3)
    vy_along_x = forward_diff(vel_y, 2)
    sig_xy = sig_xy + time_step * shear_mu * (vx_along_y + vy_along_x)
    sig_xz = sig_xz + time_step * shear_mu * (vx_up + vz_along_x)
    sig_yz = sig_yz + time_step * shear_mu * (vy_up + vz_along_y)
    rotation = (vz_along_y - vy_up) + (vx_up - vz_along_x) + (vy_along_x - vx_along_y)
    return [vel_x, vel_y, vel_z, sig_xx, sig_yy, sig_zz, sig_xy, sig_xz, sig_yz], rotation


def reference(wavefields, earth_model, source_depth, source_column, wavelet, receiver_depth, receiver_column, traces):
    buoyancy = earth_model[0]
    lame_lambda = earth_model[1]
    shear_mu = earth_model[2]
    image_pp = jnp.zeros((NZ, NX, NY), jnp.float32)
    image_ps = jnp.zeros((NZ, NX, NY), jnp.float32)
    zero_plane = jnp.zeros((2, NX, NY), jnp.float32)
    for shot_index in range(SHOTS):
        fields = [wavefields[shot_index, :, field_no] for field_no in range(9)]
        src_row = source_column[shot_index] // NY
        src_col = source_column[shot_index] % NY
        rec_row = receiver_column[shot_index] // NY
        rec_col = receiver_column[shot_index] % NY
        for step_index in range(STEPS):
            vel_x, vel_y, vel_z = velocity_half(fields, buoyancy, zero_plane, zero_plane, zero_plane)
            vel_z = vel_z.at[1, receiver_depth[shot_index], rec_row, rec_col].add(time_step * traces[shot_index, step_index])
            fields, rotation = stress_half([vel_x, vel_y, vel_z] + list(fields[3:]), lame_lambda, shear_mu, zero_plane, zero_plane, zero_plane)
            for field_no in (3, 4, 5):
                fields[field_no] = fields[field_no].at[0, source_depth[shot_index], src_row, src_col].add(time_step * wavelet[shot_index, step_index])
            pressure = (fields[3] + fields[4] + fields[5]) / 3.0
            image_pp = image_pp + pressure[0] * pressure[1]
            image_ps = image_ps + pressure[0] * rotation[1]
    return jnp.stack([image_pp, image_ps]) / STEPS
```

```python
import functools

import jax
import jax.numpy as jnp
from jax import lax
from jax.experimental import pallas as pl
from jax.experimental.pallas import tpu as pltpu
from jax.sharding import PartitionSpec as P

time_step = 0.15
VX, VY, VZ, SXX, SYY, SZZ, SXY, SXZ, SYZ = range(9)
MESH = pl.DeviceIdType.MESH


def kernel(
    gz_count,
    shot_count,
    wave_hbm,
    earth_hbm,
    src_depth_hbm,
    src_column_hbm,
    wavelet_hbm,
    rec_depth_hbm,
    rec_column_hbm,
    traces_hbm,
    out,
    state,
    earth,
    low0,
    high0,
    earth_low,
    earth_high,
    low,
    high,
    send_low,
    send_high,
    inject,
    press,
    image,
    parts_in,
    own,
    src_depth,
    src_column,
    wavelet,
    rec_depth,
    rec_column,
    traces,
    load_sem,
    init_send,
    init_recv,
    low_send,
    low_recv,
    high_send,
    high_recv,
    img_send,
    img_recv,
):
    planes, nx, ny = state.shape[2:]
    steps = traces.shape[0]
    h = time_step
    gz = lax.axis_index("gz")
    shot = lax.axis_index("shot")
    has_low = gz > 0
    has_high = gz < gz_count - 1

    load_wave = [
        pltpu.make_async_copy(wave_hbm.at[0, w], state.at[w], load_sem.at[w]) for w in range(2)
    ]
    load_earth = pltpu.make_async_copy(earth_hbm, earth, load_sem.at[2])
    small = [
        pltpu.make_async_copy(src, dst, load_sem.at[3 + i])
        for i, (src, dst) in enumerate(
            (
                (traces_hbm.at[0], traces),
                (rec_depth_hbm, rec_depth),
                (rec_column_hbm, rec_column),
                (src_depth_hbm, src_depth),
                (src_column_hbm, src_column),
                (wavelet_hbm, wavelet),
            )
        )
    ]
    for copy in small + [load_earth] + load_wave:
        copy.start()

    barrier = pltpu.get_barrier_semaphore()

    @pl.when(has_low)
    def _():
        pl.semaphore_signal(barrier, inc=1, device_id={"gz": gz - 1}, device_id_type=MESH)

    @pl.when(has_high)
    def _():
        pl.semaphore_signal(barrier, inc=1, device_id={"gz": gz + 1}, device_id_type=MESH)

    for k in range(1, shot_count):
        peer = lax.rem(shot + k, shot_count)
        pl.semaphore_signal(barrier, inc=1, device_id={"shot": peer}, device_id_type=MESH)

    low_peers = (gz + gz_count - 1) // gz_count
    high_peers = (2 * gz_count - 2 - gz) // gz_count
    pl.semaphore_wait(barrier, low_peers + high_peers + shot_count - 1)

    def remote(src, dst, sem, axis_to):
        return pltpu.make_async_remote_copy(
            src_ref=src,
            dst_ref=dst,
            send_sem=init_send.at[sem],
            recv_sem=init_recv.at[sem],
            device_id={"gz": axis_to},
            device_id_type=MESH,
        )

    last = planes - 1
    down = {
        w: [
            remote(wave_hbm.at[0, w, pl.ds(SXZ, 2), last], low0.at[w, pl.ds(2, 2)], 6 * w, gz + 1),
            remote(wave_hbm.at[0, w, SZZ, last], low0.at[w, 1], 6 * w + 1, gz + 1),
            remote(wave_hbm.at[0, w, VZ, last], low0.at[w, 0], 6 * w + 2, gz + 1),
        ]
        for w in range(2)
    }
    down_earth = remote(earth_hbm.at[0, last], earth_low, 12, gz + 1)
    up = {
        w: [
            remote(wave_hbm.at[0, w, pl.ds(SXX, 6), 0], high0.at[w, pl.ds(SXX, 6)], 6 * w + 3, gz - 1),
            remote(wave_hbm.at[0, w, pl.ds(VX, 2), 0], high0.at[w, pl.ds(VX, 2)], 6 * w + 4, gz - 1),
        ]
        for w in range(2)
    }
    up_earth = remote(earth_hbm.at[:, 0], earth_high, 13, gz - 1)
    down_all = down[0] + [down_earth] + down[1]
    up_all = up[0] + [up_earth] + up[1]

    @pl.when(has_high)
    def _():
        for copy in down_all:
            copy.start()

    @pl.when(has_low)
    def _():
        for copy in up_all:
            copy.start()

    @pl.when(jnp.logical_not(has_low))
    def _():
        low0[...] = jnp.zeros_like(low0)
        low[...] = jnp.zeros_like(low)
        earth_low[...] = jnp.zeros_like(earth_low)

    @pl.when(jnp.logical_not(has_high))
    def _():
        high0[...] = jnp.zeros_like(high0)
        high[...] = jnp.zeros_like(high)
        earth_high[...] = jnp.zeros_like(earth_high)

    image[...] = jnp.zeros_like(image)

    for copy in small:
        copy.wait()
    offset = gz * planes
    receivers = traces.shape[1]
    column = rec_column[...]
    depth = rec_depth[...] - offset
    row_ids = lax.broadcasted_iota(jnp.int32, (nx, receivers), 0) * ny
    past = column - row_ids
    on_row = (past >= 0) & (past < ny)
    row_hot = jnp.concatenate(
        [jnp.where(on_row & (depth == p), h, 0.0) for p in range(-1, planes)], axis=0
    )
    col_ids = lax.broadcasted_iota(jnp.int32, (ny, receivers), 0)
    col_hot = jnp.where((column & (ny - 1)) == col_ids, 1.0, 0.0)

    def fill(n, carry):
        inject[n] = lax.dot_general(
            row_hot * traces[pl.ds(n, 1), :],
            col_hot,
            (((1,), (1,)), ((), ())),
            precision=lax.Precision.HIGHEST,
            preferred_element_type=jnp.float32,
        ).reshape(planes + 1, nx, ny)
        return carry

    lax.fori_loop(0, steps, fill, 0)

    rows = lax.broadcasted_iota(jnp.int32, (nx, ny), 0)
    lanes = lax.broadcasted_iota(jnp.int32, (nx, ny), 1)
    cells = rows * ny + lanes

    def fx(a):
        return jnp.where(rows == nx - 1, 0.0, pltpu.roll(a, nx - 1, 0)) - a

    def bx(a):
        return a - jnp.where(rows == 0, 0.0, pltpu.roll(a, 1, 0))

    def fy(a):
        return jnp.where(lanes == ny - 1, 0.0, pltpu.roll(a, ny - 1, 1)) - a

    def by(a):
        return a - jnp.where(lanes == 0, 0.0, pltpu.roll(a, 1, 1))

    src_at = src_depth[0] - offset
    src_cell = src_column[0]

    def source_term(plane, n):
        cell = jnp.where(src_at == plane, src_cell, -1)
        return jnp.where(cells == cell, h * wavelet[0, n], 0.0)

    load_earth.wait()
    earth[...] = earth[...] * h

    def sends(w, n):
        to_high = pltpu.make_async_remote_copy(
            src_ref=send_low.at[w, n],
            dst_ref=low.at[w, n],
            send_sem=low_send.at[w, n],
            recv_sem=low_recv.at[w, n],
            device_id={"gz": gz + 1},
            device_id_type=MESH,
        )
        to_low = pltpu.make_async_remote_copy(
            src_ref=send_high.at[w, n],
            dst_ref=high.at[w, n],
            send_sem=high_send.at[w, n],
            recv_sem=high_recv.at[w, n],
            device_id={"gz": gz - 1},
            device_id_type=MESH,
        )
        return to_high, to_low

    def half(w, n, first, final):
        if first:
            load_wave[w].wait()

            @pl.when(has_low)
            def _():
                for copy in down[w]:
                    copy.wait_recv()
                if w == 0:
                    down_earth.wait_recv()

            @pl.when(has_high)
            def _():
                for copy in up[w]:
                    copy.wait_recv()
                if w == 0:
                    up_earth.wait_recv()

            szz_m, sxz_m, syz_m = (low0[w, i] for i in (1, 2, 3))
            sxz_p, syz_p = high0[w, SXZ], high0[w, SYZ]
        else:
            to_high, to_low = sends(w, n - 1)

            @pl.when(has_high)
            def _():
                to_low.wait_recv()

            @pl.when(has_low)
            def _():
                to_high.wait_recv()

            szz_m, sxz_m, syz_m = (low[w, n - 1, i] for i in range(3))
            vz_p, sxz_p, syz_p = (high[w, n - 1, i] for i in range(3))
            hlam = h * earth_high[1]
            hmu = h * earth_high[2]
            vx_p, vy_p = high0[w, VX], high0[w, VY]
            ex, ey, ez = bx(vx_p), by(vy_p), vz_p - state[w, VZ, last]
            spread = hlam * (ex + ey + ez)
            if w == 0:
                spread = spread + source_term(planes, n - 1)
            high0[w, SXX] += spread + 2.0 * hmu * ex
            high0[w, SYY] += spread + 2.0 * hmu * ey
            high0[w, SZZ] += spread + 2.0 * hmu * ez
            high0[w, SXY] += hmu * (fy(vx_p) + fx(vy_p))

        term = h * earth_low[...] * (bx(sxz_m) + by(syz_m) + (state[w, SZZ, 0] - szz_m))
        if w == 1:
            term = term + inject[n, 0]
        low0[w, 0] += term
        for p in range(planes):
            hb = earth[0, p]
            sxz, syz, szz, sxy = (state[w, i, p] for i in (SXZ, SYZ, SZZ, SXY))
            sxz_b = sxz_m if p == 0 else state[w, SXZ, p - 1]
            syz_b = syz_m if p == 0 else state[w, SYZ, p - 1]
            szz_f = high0[w, SZZ] if p == last else state[w, SZZ, p + 1]
            state[w, VX, p] += hb * (fx(state[w, SXX, p]) + by(sxy) + (sxz - sxz_b))
            state[w, VY, p] += hb * (bx(sxy) + fy(state[w, SYY, p]) + (syz - syz_b))
            term = hb * (bx(sxz) + by(syz) + (szz_f - szz))
            if w == 1:
                term = term + inject[n, p + 1]
            state[w, VZ, p] += term
        hb = h * earth_high[0]
        sxy = high0[w, SXY]
        high0[w, VX] += hb * (fx(high0[w, SXX]) + by(sxy) + (sxz_p - state[w, SXZ, last]))
        high0[w, VY] += hb * (bx(sxy) + fy(high0[w, SYY]) + (syz_p - state[w, SYZ, last]))

        def stress(p):
            vx, vy, vz = (state[w, i, p] for i in (VX, VY, VZ))
            vz_b = low0[w, 0] if p == 0 else state[w, VZ, p - 1]
            hmu = earth[2, p]
            ex, ey, ez = bx(vx), by(vy), vz - vz_b
            spread = earth[1, p] * (ex + ey + ez)
            if w == 0:
                spread = spread + source_term(p, n)
            mu2 = 2.0 * hmu
            sxx = state[w, SXX, p] + (spread + mu2 * ex)
            syy = state[w, SYY, p] + (spread + mu2 * ey)
            szz = state[w, SZZ, p] + (spread + mu2 * ez)
            pressure = (sxx + syy + szz) * (1.0 / 3.0)
            if not final:
                state[w, SXX, p] = sxx
                state[w, SYY, p] = syy
                state[w, SZZ, p] = szz
            if w == 1 or not final:
                vx_f = high0[w, VX] if p == last else state[w, VX, p + 1]
                vy_f = high0[w, VY] if p == last else state[w, VY, p + 1]
                vxz, vyz = vx_f - vx, vy_f - vy
                vzx, vzy, vxy, vyx = fx(vz), fy(vz), fy(vx), fx(vy)
            if not final:
                sxz = state[w, SXZ, p] + hmu * (vxz + vzx)
                syz = state[w, SYZ, p] + hmu * (vyz + vzy)
                state[w, SXY, p] += hmu * (vxy + vyx)
                state[w, SXZ, p] = sxz
                state[w, SYZ, p] = syz
                if p == 0:
                    send_high[w, n, 0] = vz
                    send_high[w, n, 1] = sxz
                    send_high[w, n, 2] = syz
                if p == last:
                    send_low[w, n, 0] = szz
                    send_low[w, n, 1] = sxz
                    send_low[w, n, 2] = syz
            if w == 0:
                press[p] = pressure
            else:
                rotation = (vzy - vyz) + (vxz - vzx) + (vyx - vxy)
                image[pl.ds(p * nx, nx), :] += press[p] * pressure
                image[pl.ds((planes + p) * nx, nx), :] += press[p] * rotation

        edge = sorted({0, last})
        for p in edge:
            stress(p)
        if not final:
            to_high, to_low = sends(w, n)

            @pl.when(has_low)
            def _():
                to_low.start()

            @pl.when(has_high)
            def _():
                to_high.start()

        for p in range(planes):
            if p not in edge:
                stress(p)

    def step(n, first, final):
        half(0, n, first, final)
        half(1, n, first, final)

    step(0, True, steps == 1)
    if steps > 2:

        def body(n, carry):
            step(n, False, False)
            return carry

        lax.fori_loop(1, steps - 1, body, 0)
    if steps > 1:
        step(steps - 1, False, True)

    total = image.shape[0]
    chunk = total // shot_count
    scale = 1.0 / steps

    def span(index):
        return pl.ds(pl.multiple_of(index * chunk, 8), chunk)

    scatter = []
    for k in range(1, shot_count):
        peer = lax.rem(shot + k, shot_count)
        copy = pltpu.make_async_remote_copy(
            src_ref=image.at[span(peer)],
            dst_ref=parts_in.at[k - 1],
            send_sem=img_send.at[0, k - 1],
            recv_sem=img_recv.at[0, k - 1],
            device_id={"shot": peer},
            device_id_type=MESH,
        )
        copy.start()
        scatter.append(copy)
    acc = image[span(shot), :]
    for k in range(1, shot_count):
        scatter[k - 1].wait_recv()
        acc = acc + parts_in[k - 1]
    acc = acc * scale
    own[...] = acc
    gather = []
    for k in range(1, shot_count):
        peer = lax.rem(shot + k, shot_count)
        copy = pltpu.make_async_remote_copy(
            src_ref=own,
            dst_ref=out.at[span(shot)],
            send_sem=img_send.at[1, k - 1],
            recv_sem=img_recv.at[1, k - 1],
            device_id={"shot": peer},
            device_id_type=MESH,
        )
        copy.start()
        gather.append(copy)
    out[span(shot), :] = acc

    @pl.when(has_high)
    def _():
        for copy in down_all:
            copy.wait_send()

    @pl.when(has_low)
    def _():
        for copy in up_all:
            copy.wait_send()

    def drain(n, carry):
        for w in range(2):
            to_high, to_low = sends(w, n)

            @pl.when(has_high)
            def _():
                to_high.wait_send()

            @pl.when(has_low)
            def _():
                to_low.wait_send()

        return carry

    lax.fori_loop(0, steps - 1, drain, 0)
    for copy in scatter:
        copy.wait_send()
    for copy in gather:
        copy.wait()


def on_device(
    gz_count,
    shot_count,
    wavefields,
    earth_model,
    source_depth,
    source_column,
    wavelet,
    receiver_depth,
    receiver_column,
    traces,
):
    planes, nx, ny = wavefields.shape[3:]
    steps = wavelet.shape[1]
    slots = max(steps - 1, 1)
    rows = 2 * planes * nx
    peers = max(shot_count - 1, 1)
    f32 = jnp.float32
    vmem = pl.BlockSpec(memory_space=pltpu.VMEM)
    hbm = pl.BlockSpec(memory_space=pl.ANY)
    dma = pltpu.SemaphoreType.DMA
    summed = pl.pallas_call(
        functools.partial(kernel, gz_count, shot_count),
        out_shape=jax.ShapeDtypeStruct((rows, ny), f32),
        in_specs=[hbm] * 8,
        out_specs=vmem,
        scratch_shapes=[
            pltpu.VMEM((2, 9, planes, nx, ny), f32),
            pltpu.VMEM((3, planes, nx, ny), f32),
            pltpu.VMEM((2, 4, nx, ny), f32),
            pltpu.VMEM((2, 9, nx, ny), f32),
            pltpu.VMEM((nx, ny), f32),
            pltpu.VMEM((3, nx, ny), f32),
            pltpu.VMEM((2, slots, 3, nx, ny), f32),
            pltpu.VMEM((2, slots, 3, nx, ny), f32),
            pltpu.VMEM((2, slots, 3, nx, ny), f32),
            pltpu.VMEM((2, slots, 3, nx, ny), f32),
            pltpu.VMEM((steps, planes + 1, nx, ny), f32),
            pltpu.VMEM((planes, nx, ny), f32),
            pltpu.VMEM((rows, ny), f32),
            pltpu.VMEM((peers, rows // shot_count, ny), f32),
            pltpu.VMEM((rows // shot_count, ny), f32),
            pltpu.SMEM(source_depth.shape, jnp.int32),
            pltpu.SMEM(source_column.shape, jnp.int32),
            pltpu.SMEM(wavelet.shape, f32),
            pltpu.VMEM(receiver_depth.shape, jnp.int32),
            pltpu.VMEM(receiver_column.shape, jnp.int32),
            pltpu.VMEM(traces.shape[1:], f32),
            dma((9,)),
            dma((14,)),
            dma((14,)),
            dma((2, slots)),
            dma((2, slots)),
            dma((2, slots)),
            dma((2, slots)),
            dma((2, peers)),
            dma((2, peers)),
        ],
        compiler_params=pltpu.CompilerParams(collective_id=0, has_side_effects=True),
    )(
        wavefields,
        earth_model,
        source_depth,
        source_column,
        wavelet,
        receiver_depth,
        receiver_column,
        traces,
    )
    return summed.reshape(2, planes, nx, ny)


def solution(mesh):
    placed = (
        P(("parts", "shot"), None, None, "gz", None, None),
        P("parts", "gz", None, None),
        P(("parts", "shot")),
        P(("parts", "shot")),
        P(("parts", "shot"), None),
        P(("parts", "shot"), None),
        P(("parts", "shot"), None),
        P(("parts", "shot"), None, None),
    )
    return jax.shard_map(
        functools.partial(on_device, mesh.shape["gz"], mesh.shape["shot"]),
        mesh=mesh,
        in_specs=placed,
        out_specs=P("parts", "gz", None, None),
        check_vma=False,
    )
```

```python
import functools

import jax
import jax.numpy as jnp
from jax import lax
from jax.experimental import pallas as pl
from jax.experimental.pallas import tpu as pltpu
from jax.sharding import PartitionSpec as P

time_step = 0.15
VX, VY, VZ, SXX, SYY, SZZ, SXY, SXZ, SYZ = range(9)
MESH = pl.DeviceIdType.MESH


def kernel(
    gz_count,
    shot_count,
    wave_hbm,
    earth_hbm,
    src_depth_hbm,
    src_column_hbm,
    wavelet_hbm,
    rec_depth_hbm,
    rec_column_hbm,
    traces_hbm,
    out,
    state,
    earth,
    low0,
    high0,
    earth_low,
    earth_high,
    low,
    high,
    send_low,
    send_high,
    inject,
    press,
    image,
    parts_in,
    own,
    src_depth,
    src_column,
    wavelet,
    rec_depth,
    rec_column,
    traces,
    load_sem,
    init_send,
    init_recv,
    low_send,
    low_recv,
    high_send,
    high_recv,
    img_send,
    img_recv,
    turn,
):
    planes, nx, ny = state.shape[2:]
    steps = traces.shape[0]
    h = time_step
    gz = lax.axis_index("gz")
    shot = lax.axis_index("shot")
    has_low = gz > 0
    has_high = gz < gz_count - 1

    load_wave = [
        pltpu.make_async_copy(wave_hbm.at[0, w], state.at[w], load_sem.at[w]) for w in range(2)
    ]
    load_earth = pltpu.make_async_copy(earth_hbm, earth, load_sem.at[2])
    small = [
        pltpu.make_async_copy(src, dst, load_sem.at[3 + i])
        for i, (src, dst) in enumerate(
            (
                (traces_hbm.at[0], traces),
                (rec_depth_hbm, rec_depth),
                (rec_column_hbm, rec_column),
                (src_depth_hbm, src_depth),
                (src_column_hbm, src_column),
                (wavelet_hbm, wavelet),
            )
        )
    ]
    for copy in small + [load_earth] + load_wave:
        copy.start()

    barrier = pltpu.get_barrier_semaphore()

    @pl.when(has_low)
    def _():
        pl.semaphore_signal(barrier, inc=1, device_id={"gz": gz - 1}, device_id_type=MESH)

    @pl.when(has_high)
    def _():
        pl.semaphore_signal(barrier, inc=1, device_id={"gz": gz + 1}, device_id_type=MESH)

    for k in range(1, shot_count):
        peer = lax.rem(shot + k, shot_count)
        pl.semaphore_signal(barrier, inc=1, device_id={"shot": peer}, device_id_type=MESH)

    low_peers = (gz + gz_count - 1) // gz_count
    high_peers = (2 * gz_count - 2 - gz) // gz_count
    pl.semaphore_wait(barrier, low_peers + high_peers + shot_count - 1)

    def remote(src, dst, sem, axis_to):
        return pltpu.make_async_remote_copy(
            src_ref=src,
            dst_ref=dst,
            send_sem=init_send.at[sem],
            recv_sem=init_recv.at[sem],
            device_id={"gz": axis_to},
            device_id_type=MESH,
        )

    last = planes - 1
    down = {
        w: [
            remote(wave_hbm.at[0, w, pl.ds(SXZ, 2), last], low0.at[w, pl.ds(2, 2)], 6 * w, gz + 1),
            remote(wave_hbm.at[0, w, SZZ, last], low0.at[w, 1], 6 * w + 1, gz + 1),
            remote(wave_hbm.at[0, w, VZ, last], low0.at[w, 0], 6 * w + 2, gz + 1),
        ]
        for w in range(2)
    }
    down_earth = remote(earth_hbm.at[0, last], earth_low, 12, gz + 1)
    up = {
        w: [
            remote(wave_hbm.at[0, w, pl.ds(SXX, 6), 0], high0.at[w, pl.ds(SXX, 6)], 6 * w + 3, gz - 1),
            remote(wave_hbm.at[0, w, pl.ds(VX, 2), 0], high0.at[w, pl.ds(VX, 2)], 6 * w + 4, gz - 1),
        ]
        for w in range(2)
    }
    up_earth = remote(earth_hbm.at[:, 0], earth_high, 13, gz - 1)
    down_all = down[0] + [down_earth] + down[1]
    up_all = up[0] + [up_earth] + up[1]

    def start_first():
        @pl.when(has_high)
        def _():
            for copy in down_all:
                copy.start()

        @pl.when(has_low)
        def _():
            for copy in up_all:
                copy.start()

    paired = shot_count % 2 == 0
    even = lax.rem(shot, 2) == 0
    if paired:
        pl.when(even)(start_first)
    else:
        start_first()

    @pl.when(jnp.logical_not(has_low))
    def _():
        low0[...] = jnp.zeros_like(low0)
        low[...] = jnp.zeros_like(low)
        earth_low[...] = jnp.zeros_like(earth_low)

    @pl.when(jnp.logical_not(has_high))
    def _():
        high0[...] = jnp.zeros_like(high0)
        high[...] = jnp.zeros_like(high)
        earth_high[...] = jnp.zeros_like(earth_high)

    image[...] = jnp.zeros_like(image)

    for copy in small:
        copy.wait()
    offset = gz * planes
    receivers = traces.shape[1]
    column = rec_column[...]
    depth = rec_depth[...] - offset
    row_ids = lax.broadcasted_iota(jnp.int32, (nx, receivers), 0) * ny
    past = column - row_ids
    on_row = (past >= 0) & (past < ny)
    row_hot = jnp.concatenate(
        [jnp.where(on_row & (depth == p), h, 0.0) for p in range(-1, planes)], axis=0
    )
    col_ids = lax.broadcasted_iota(jnp.int32, (ny, receivers), 0)
    col_hot = jnp.where((column & (ny - 1)) == col_ids, 1.0, 0.0)

    def fill(n, carry):
        inject[n] = lax.dot_general(
            row_hot * traces[pl.ds(n, 1), :],
            col_hot,
            (((1,), (1,)), ((), ())),
            precision=lax.Precision.HIGHEST,
            preferred_element_type=jnp.float32,
        ).reshape(planes + 1, nx, ny)
        return carry

    lax.fori_loop(0, steps, fill, 0)

    if paired:

        @pl.when(even)
        def _():
            @pl.when(has_high)
            def _():
                for copy in down_all:
                    copy.wait_send()

            @pl.when(has_low)
            def _():
                for copy in up_all:
                    copy.wait_send()

            pl.semaphore_signal(turn, inc=1, device_id={"shot": shot + 1}, device_id_type=MESH)

        @pl.when(jnp.logical_not(even))
        def _():
            pl.semaphore_wait(turn, 1)
            start_first()

    rows = lax.broadcasted_iota(jnp.int32, (nx, ny), 0)
    lanes = lax.broadcasted_iota(jnp.int32, (nx, ny), 1)
    cells = rows * ny + lanes

    def fx(a):
        return jnp.where(rows == nx - 1, 0.0, pltpu.roll(a, nx - 1, 0)) - a

    def bx(a):
        return a - jnp.where(rows == 0, 0.0, pltpu.roll(a, 1, 0))

    def fy(a):
        return jnp.where(lanes == ny - 1, 0.0, pltpu.roll(a, ny - 1, 1)) - a

    def by(a):
        return a - jnp.where(lanes == 0, 0.0, pltpu.roll(a, 1, 1))

    src_at = src_depth[0] - offset
    src_cell = src_column[0]

    def source_term(plane, n):
        cell = jnp.where(src_at == plane, src_cell, -1)
        return jnp.where(cells == cell, h * wavelet[0, n], 0.0)

    load_earth.wait()
    earth[...] = earth[...] * h

    def sends(w, n):
        to_high = pltpu.make_async_remote_copy(
            src_ref=send_low.at[w, n],
            dst_ref=low.at[w, n],
            send_sem=low_send.at[w, n],
            recv_sem=low_recv.at[w, n],
            device_id={"gz": gz + 1},
            device_id_type=MESH,
        )
        to_low = pltpu.make_async_remote_copy(
            src_ref=send_high.at[w, n],
            dst_ref=high.at[w, n],
            send_sem=high_send.at[w, n],
            recv_sem=high_recv.at[w, n],
            device_id={"gz": gz - 1},
            device_id_type=MESH,
        )
        return to_high, to_low

    def half(w, n, first, final):
        if first:
            load_wave[w].wait()

            @pl.when(has_low)
            def _():
                for copy in down[w]:
                    copy.wait_recv()
                if w == 0:
                    down_earth.wait_recv()

            @pl.when(has_high)
            def _():
                for copy in up[w]:
                    copy.wait_recv()
                if w == 0:
                    up_earth.wait_recv()

            szz_m, sxz_m, syz_m = (low0[w, i] for i in (1, 2, 3))
            sxz_p, syz_p = high0[w, SXZ], high0[w, SYZ]
        else:
            to_high, to_low = sends(w, n - 1)

            @pl.when(has_high)
            def _():
                to_low.wait_recv()

            @pl.when(has_low)
            def _():
                to_high.wait_recv()

            szz_m, sxz_m, syz_m = (low[w, n - 1, i] for i in range(3))
            vz_p, sxz_p, syz_p = (high[w, n - 1, i] for i in range(3))
            hlam = h * earth_high[1]
            hmu = h * earth_high[2]
            vx_p, vy_p = high0[w, VX], high0[w, VY]
            ex, ey, ez = bx(vx_p), by(vy_p), vz_p - state[w, VZ, last]
            spread = hlam * (ex + ey + ez)
            if w == 0:
                spread = spread + source_term(planes, n - 1)
            high0[w, SXX] += spread + 2.0 * hmu * ex
            high0[w, SYY] += spread + 2.0 * hmu * ey
            high0[w, SZZ] += spread + 2.0 * hmu * ez
            high0[w, SXY] += hmu * (fy(vx_p) + fx(vy_p))

        term = h * earth_low[...] * (bx(sxz_m) + by(syz_m) + (state[w, SZZ, 0] - szz_m))
        if w == 1:
            term = term + inject[n, 0]
        low0[w, 0] += term
        for p in range(planes):
            hb = earth[0, p]
            sxz, syz, szz, sxy = (state[w, i, p] for i in (SXZ, SYZ, SZZ, SXY))
            sxz_b = sxz_m if p == 0 else state[w, SXZ, p - 1]
            syz_b = syz_m if p == 0 else state[w, SYZ, p - 1]
            szz_f = high0[w, SZZ] if p == last else state[w, SZZ, p + 1]
            state[w, VX, p] += hb * (fx(state[w, SXX, p]) + by(sxy) + (sxz - sxz_b))
            state[w, VY, p] += hb * (bx(sxy) + fy(state[w, SYY, p]) + (syz - syz_b))
            term = hb * (bx(sxz) + by(syz) + (szz_f - szz))
            if w == 1:
                term = term + inject[n, p + 1]
            state[w, VZ, p] += term
        hb = h * earth_high[0]
        sxy = high0[w, SXY]
        high0[w, VX] += hb * (fx(high0[w, SXX]) + by(sxy) + (sxz_p - state[w, SXZ, last]))
        high0[w, VY] += hb * (bx(sxy) + fy(high0[w, SYY]) + (syz_p - state[w, SYZ, last]))

        def stress(p):
            vx, vy, vz = (state[w, i, p] for i in (VX, VY, VZ))
            vz_b = low0[w, 0] if p == 0 else state[w, VZ, p - 1]
            hmu = earth[2, p]
            ex, ey, ez = bx(vx), by(vy), vz - vz_b
            spread = earth[1, p] * (ex + ey + ez)
            if w == 0:
                spread = spread + source_term(p, n)
            mu2 = 2.0 * hmu
            sxx = state[w, SXX, p] + (spread + mu2 * ex)
            syy = state[w, SYY, p] + (spread + mu2 * ey)
            szz = state[w, SZZ, p] + (spread + mu2 * ez)
            pressure = (sxx + syy + szz) * (1.0 / 3.0)
            if not final:
                state[w, SXX, p] = sxx
                state[w, SYY, p] = syy
                state[w, SZZ, p] = szz
            if w == 1 or not final:
                vx_f = high0[w, VX] if p == last else state[w, VX, p + 1]
                vy_f = high0[w, VY] if p == last else state[w, VY, p + 1]
                vxz, vyz = vx_f - vx, vy_f - vy
                vzx, vzy, vxy, vyx = fx(vz), fy(vz), fy(vx), fx(vy)
            if not final:
                sxz = state[w, SXZ, p] + hmu * (vxz + vzx)
                syz = state[w, SYZ, p] + hmu * (vyz + vzy)
                state[w, SXY, p] += hmu * (vxy + vyx)
                state[w, SXZ, p] = sxz
                state[w, SYZ, p] = syz
                if p == 0:
                    send_high[w, n, 0] = vz
                    send_high[w, n, 1] = sxz
                    send_high[w, n, 2] = syz
                if p == last:
                    send_low[w, n, 0] = szz
                    send_low[w, n, 1] = sxz
                    send_low[w, n, 2] = syz
            if w == 0:
                press[p] = pressure
            else:
                rotation = (vzy - vyz) + (vxz - vzx) + (vyx - vxy)
                image[pl.ds(p * nx, nx), :] += press[p] * pressure
                image[pl.ds((planes + p) * nx, nx), :] += press[p] * rotation

        edge = sorted({0, last})
        for p in edge:
            stress(p)
        if not final:
            to_high, to_low = sends(w, n)

            @pl.when(has_low)
            def _():
                to_low.start()

            @pl.when(has_high)
            def _():
                to_high.start()

        for p in range(planes):
            if p not in edge:
                stress(p)

    def step(n, first, final):
        half(0, n, first, final)
        half(1, n, first, final)

    step(0, True, steps == 1)
    if steps > 2:

        def body(n, carry):
            step(n, False, False)
            return carry

        lax.fori_loop(1, steps - 1, body, 0)
    if steps > 1:
        step(steps - 1, False, True)

    total = image.shape[0]
    chunk = total // shot_count
    scale = 1.0 / steps

    def span(index):
        return pl.ds(pl.multiple_of(index * chunk, 8), chunk)

    scatter = []
    for k in range(1, shot_count):
        peer = lax.rem(shot + k, shot_count)
        copy = pltpu.make_async_remote_copy(
            src_ref=image.at[span(peer)],
            dst_ref=parts_in.at[k - 1],
            send_sem=img_send.at[0, k - 1],
            recv_sem=img_recv.at[0, k - 1],
            device_id={"shot": peer},
            device_id_type=MESH,
        )
        copy.start()
        scatter.append(copy)
    acc = image[span(shot), :]
    for k in range(1, shot_count):
        scatter[k - 1].wait_recv()
        acc = acc + parts_in[k - 1]
    acc = acc * scale
    own[...] = acc
    gather = []
    for k in range(1, shot_count):
        peer = lax.rem(shot + k, shot_count)
        copy = pltpu.make_async_remote_copy(
            src_ref=own,
            dst_ref=out.at[span(shot)],
            send_sem=img_send.at[1, k - 1],
            recv_sem=img_recv.at[1, k - 1],
            device_id={"shot": peer},
            device_id_type=MESH,
        )
        copy.start()
        gather.append(copy)
    out[span(shot), :] = acc

    late = jnp.logical_not(even) if paired else shot >= 0

    @pl.when(has_high & late)
    def _():
        for copy in down_all:
            copy.wait_send()

    @pl.when(has_low & late)
    def _():
        for copy in up_all:
            copy.wait_send()

    def drain(n, carry):
        for w in range(2):
            to_high, to_low = sends(w, n)

            @pl.when(has_high)
            def _():
                to_high.wait_send()

            @pl.when(has_low)
            def _():
                to_low.wait_send()

        return carry

    lax.fori_loop(0, steps - 1, drain, 0)
    for copy in scatter:
        copy.wait_send()
    for copy in gather:
        copy.wait()


def on_device(
    gz_count,
    shot_count,
    wavefields,
    earth_model,
    source_depth,
    source_column,
    wavelet,
    receiver_depth,
    receiver_column,
    traces,
):
    planes, nx, ny = wavefields.shape[3:]
    steps = wavelet.shape[1]
    slots = max(steps - 1, 1)
    rows = 2 * planes * nx
    peers = max(shot_count - 1, 1)
    f32 = jnp.float32
    vmem = pl.BlockSpec(memory_space=pltpu.VMEM)
    hbm = pl.BlockSpec(memory_space=pl.ANY)
    dma = pltpu.SemaphoreType.DMA
    summed = pl.pallas_call(
        functools.partial(kernel, gz_count, shot_count),
        out_shape=jax.ShapeDtypeStruct((rows, ny), f32),
        in_specs=[hbm] * 8,
        out_specs=vmem,
        scratch_shapes=[
            pltpu.VMEM((2, 9, planes, nx, ny), f32),
            pltpu.VMEM((3, planes, nx, ny), f32),
            pltpu.VMEM((2, 4, nx, ny), f32),
            pltpu.VMEM((2, 9, nx, ny), f32),
            pltpu.VMEM((nx, ny), f32),
            pltpu.VMEM((3, nx, ny), f32),
            pltpu.VMEM((2, slots, 3, nx, ny), f32),
            pltpu.VMEM((2, slots, 3, nx, ny), f32),
            pltpu.VMEM((2, slots, 3, nx, ny), f32),
            pltpu.VMEM((2, slots, 3, nx, ny), f32),
            pltpu.VMEM((steps, planes + 1, nx, ny), f32),
            pltpu.VMEM((planes, nx, ny), f32),
            pltpu.VMEM((rows, ny), f32),
            pltpu.VMEM((peers, rows // shot_count, ny), f32),
            pltpu.VMEM((rows // shot_count, ny), f32),
            pltpu.SMEM(source_depth.shape, jnp.int32),
            pltpu.SMEM(source_column.shape, jnp.int32),
            pltpu.SMEM(wavelet.shape, f32),
            pltpu.VMEM(receiver_depth.shape, jnp.int32),
            pltpu.VMEM(receiver_column.shape, jnp.int32),
            pltpu.VMEM(traces.shape[1:], f32),
            dma((9,)),
            dma((14,)),
            dma((14,)),
            dma((2, slots)),
            dma((2, slots)),
            dma((2, slots)),
            dma((2, slots)),
            dma((2, peers)),
            dma((2, peers)),
            pltpu.SemaphoreType.REGULAR,
        ],
        compiler_params=pltpu.CompilerParams(collective_id=0, has_side_effects=True),
    )(
        wavefields,
        earth_model,
        source_depth,
        source_column,
        wavelet,
        receiver_depth,
        receiver_column,
        traces,
    )
    return summed.reshape(2, planes, nx, ny)


def solution(mesh):
    placed = (
        P(("parts", "shot"), None, None, "gz", None, None),
        P("parts", "gz", None, None),
        P(("parts", "shot")),
        P(("parts", "shot")),
        P(("parts", "shot"), None),
        P(("parts", "shot"), None),
        P(("parts", "shot"), None),
        P(("parts", "shot"), None, None),
    )
    return jax.shard_map(
        functools.partial(on_device, mesh.shape["gz"], mesh.shape["shot"]),
        mesh=mesh,
        in_specs=placed,
        out_specs=P("parts", "gz", None, None),
        check_vma=False,
    )
```
